32 devices in a mesh: head: 2 (over x), seq: 16 (over z, y, core).
Axes of the slice: x: 2, y: 2, z: 4, core: 2. Of those that a mesh axis runs over, the one named last changes fastest.
Arguments:
- queries: bfloat16 [8192, 4096], P('seq', 'head'), may hold values from -6 to 6
- keys: bfloat16 [8192, 4096], P('seq', 'head'), may hold values from -6 to 6
- values: bfloat16 [8192, 4096], P('seq', 'head'), may hold values from -6 to 6
- out_grad: bfloat16 [8192, 4096], P('seq', 'head'), may hold values from -8 to 8
- inputs: bfloat16 [8192, 2048], P('seq'), may hold values from -100 to 100
- momentum: float32 [2048, 4096], P('seq', 'head'), may hold values from -6 to 6
- level_weight: int32 [18, 32], replicated, may hold values from 1 to 8
Outputs:
- query_grad: bfloat16 [8192, 4096], P('seq', 'head')
- key_grad: bfloat16 [8192, 4096], P('seq', 'head')
- value_grad: bfloat16 [8192, 4096], P('seq', 'head')
- new_momentum: float32 [2048, 4096], P('seq', 'head')
The draws below stay inside these ranges and needn't reach their ends.
All inputs are finite; a program needn't handle non-finite values.
Results may differ from the reference program's by a relative error of at most 0.0095.
Values may be sent and summed in bfloat16 or wider, within the bound.
A program may use at most 128 MiB of HBM per device.

```python
import math
import jax
import jax.numpy as jnp
from jax import lax

TOK_DEV = 512
HEADS = 32
D_HEAD = 128
DX = 2048
LEVELS = 18
TOKENS = 8192
N_SEQ = 16


def draw_inputs(key, part):
    first = jax.random.fold_in(key, 11)
    second = jax.random.fold_in(key, 12)
    third = jax.random.fold_in(key, 13)
    rise = 1.0 + 2.0 * jnp.arange(DX, dtype=jnp.float32) / DX
    spread = jnp.exp(jax.random.uniform(first, (DX,), jnp.float32) * jnp.log(10.0))
    rowscale = jnp.exp(jax.random.uniform(second, (TOKENS, 1), jnp.float32) * jnp.log(10.0)) / 3.0
    noise = jax.random.truncated_normal(third, -4.0, 4.0, (TOKENS, DX), jnp.float32)
    return (noise * rowscale * rise * spread / 4.0).astype(jnp.bfloat16)


def draw_out_grad(key, part):
    first = jax.random.fold_in(key, 21)
    width = HEADS * D_HEAD
    head_of = (jnp.arange(width, dtype=jnp.int32) // D_HEAD).astype(jnp.float32)
    rise = 1.0 + head_of / max(HEADS - 1, 1)
    noise = jax.random.truncated_normal(first, -4.0, 4.0, (TOKENS, width), jnp.float32)
    return (noise * rise).astype(jnp.bfloat16)


def place_ends(result, rng, least, top_value):
    longest = result.shape.index(max(result.shape))
    spots = []
    for shift in (0, 1):
        where = [jax.random.randint(jax.random.fold_in(rng, axis), (), 0, length) for axis, length in enumerate(result.shape)]
        where[longest] = (where[longest] + shift) % result.shape[longest]
        spots.append(tuple(where))
    return result.at[spots[0]].set(least).at[spots[1]].set(top_value)


def shard_levels(stream_key, dims, split, least, high):
    gain, own = 1.0, jax.random.fold_in(stream_key, 6)
    for position, shards_of in split:
        steps = jnp.exp(jax.random.uniform(jax.random.fold_in(own, position), (shards_of,), jnp.float32, least / len(split), high / len(split)))
        gain = gain * jnp.repeat(steps, dims[position] // shards_of).reshape([-1 if axis == position else 1 for axis in range(len(dims))])
    return gain


def bell_draw(key, extent, scale, reach, shards=(), kind=jnp.bfloat16):
    entries = jax.random.normal(key, extent, jnp.float32) * scale
    if len(shards) > 0:
        entries = shard_levels(key, extent, shards, -0.22, 0.18) * entries
    return jnp.clip(entries, min=-reach, max=reach).astype(kind)


def setup_inputs(seed: int = 0) -> dict:
    splits = jax.random.split(jax.random.key(seed), 8)
    return {
        "queries": bell_draw(splits[0], (TOKENS, HEADS * D_HEAD), 1.0, 6.0, ((0, 16), (1, 2))),
        "keys": bell_draw(splits[1], (TOKENS, HEADS * D_HEAD), 1.0, 6.0, ((0, 16), (1, 2))),
        "values": bell_draw(splits[2], (TOKENS, HEADS * D_HEAD), 1.0, 6.0, ((0, 16), (1, 2))),
        "out_grad": draw_out_grad(jax.random.fold_in(splits[7], 71), 0),
        "inputs": draw_inputs(jax.random.fold_in(splits[7], 71), 0),
        "momentum": bell_draw(splits[5], (DX, HEADS * D_HEAD), 1.0, 6.0, ((0, 16), (1, 2)), jnp.float32),
        "level_weight": place_ends(jax.random.randint(splits[6], (LEVELS, HEADS), 1, 9), jax.random.fold_in(splits[6], 1), 1, 8).astype(jnp.int32),
    }


clip_norm = 1024.0
momentum_rate = 0.9

def bit_length(numbers, count):
    total = jnp.zeros_like(numbers)
    for place in range(count):
        total = total + (jnp.right_shift(numbers, place) > 0).astype(jnp.int32)
    return total

def level_table(level_weight, head_size):
    levels = jnp.arange(level_weight.shape[0], dtype=jnp.float32)
    factor = jnp.exp2(-0.5 * levels) / (8.0 * math.sqrt(head_size))
    return level_weight.astype(jnp.float32) * factor[:, None]

def lookup(level, table):
    onehot = (level[..., None] == jnp.arange(table.shape[0], dtype=jnp.int32)).astype(jnp.float32)
    flat = onehot.reshape(-1, table.shape[0])
    picked = jnp.dot(flat, table, precision=lax.Precision.HIGHEST)
    return picked.reshape(level.shape + (table.shape[1],))

def intra_weights(length, table):
    place = jnp.arange(length, dtype=jnp.int32)
    level = bit_length(jnp.bitwise_xor(place[:, None], place[None, :]), table.shape[0])
    picked = lookup(level, table)
    causal = (place[None, :] <= place[:, None])[..., None]
    return jnp.transpose(jnp.where(causal, picked, jnp.float32(0.0)), (2, 0, 1))

def span_grads(pieces, weights):
    query, key_rows, value_rows, grad_rows = [piece.astype(jnp.float32) for piece in pieces]
    scores = jnp.einsum('thd,shd->hts', query, key_rows)
    mixed = lax.optimization_barrier((weights * scores).astype(jnp.bfloat16)).astype(jnp.float32)
    value_part = jnp.einsum('hts,thd->shd', mixed, grad_rows)
    before = jnp.einsum('thd,shd->hts', grad_rows, value_rows)
    dmix = lax.optimization_barrier((weights * before).astype(jnp.bfloat16)).astype(jnp.float32)
    query_part = jnp.einsum('hts,shd->thd', dmix, key_rows)
    key_part = jnp.einsum('hts,thd->shd', dmix, query)
    return (query_part, key_part, value_part)

def reference(queries, keys, values, out_grad, inputs, momentum, level_weight):
    table = level_table(level_weight, D_HEAD)
    base_level = TOK_DEV.bit_length() - 1
    shape = (N_SEQ, TOK_DEV, HEADS, D_HEAD)
    query = queries.reshape(shape)
    key_rows = keys.reshape(shape)
    value_rows = values.reshape(shape)
    grad_rows = out_grad.reshape(shape)
    weights = intra_weights(TOK_DEV, table)

    def one_span(pieces):
        return span_grads(pieces, weights)
    query_part, key_part, value_part = lax.map(one_span, (query, key_rows, value_rows, grad_rows))
    key32 = key_rows.astype(jnp.float32)
    value32 = value_rows.astype(jnp.float32)
    query32 = query.astype(jnp.float32)
    grad32 = grad_rows.astype(jnp.float32)
    states = jnp.einsum('cthd,cthe->chde', key32, value32).astype(jnp.bfloat16)
    grads = jnp.einsum('cthd,cthe->chde', query32, grad32).astype(jnp.bfloat16)
    span = jnp.arange(N_SEQ, dtype=jnp.int32)
    level = bit_length(jnp.bitwise_xor(span[:, None], span[None, :]), table.shape[0]) + base_level
    across = jnp.where((span[None, :] < span[:, None])[..., None], lookup(level, table), jnp.float32(0.0))
    carried = jnp.einsum('ijh,jhde->ihde', across, states.astype(jnp.float32), precision=lax.Precision.HIGHEST).astype(jnp.bfloat16)
    returned = jnp.einsum('ijh,ihde->jhde', across, grads.astype(jnp.float32), precision=lax.Precision.HIGHEST).astype(jnp.bfloat16)
    carried32 = carried.astype(jnp.float32)
    returned32 = returned.astype(jnp.float32)
    width = HEADS * D_HEAD
    query_grad = (query_part + jnp.einsum('cthe,chde->cthd', grad32, carried32)).astype(jnp.bfloat16).reshape(TOKENS, width)
    key_grad = (key_part + jnp.einsum('cthe,chde->cthd', value32, returned32)).astype(jnp.bfloat16).reshape(TOKENS, width)
    value_grad = (value_part + jnp.einsum('cthd,chde->cthe', key32, returned32)).astype(jnp.bfloat16).reshape(TOKENS, width)
    proj_grad = jnp.dot(inputs.astype(jnp.float32).T, value_grad.astype(jnp.float32), precision=lax.Precision.HIGHEST, preferred_element_type=jnp.float32)
    norm = jnp.sqrt(jnp.sum(proj_grad * proj_grad) + 1e-06)
    factor = jnp.minimum(jnp.float32(1.0), clip_norm / norm)
    new_momentum = momentum_rate * momentum + factor * proj_grad
    return (query_grad, key_grad, value_grad, new_momentum)
```

```python
import math

import jax
import jax.numpy as jnp
from jax import lax
from jax.experimental import pallas as pl
from jax.experimental.pallas import tpu as pltpu
from jax.sharding import PartitionSpec as P

D_HEAD = 128


clip_norm = 1024.0
momentum_rate = 0.9


def partner(x, axis, apart):
    return lax.ppermute(x, axis, [(i, i ^ 1 << apart) for i in range(lax.axis_size(axis))])


def sum_everywhere(x, axes):
    for axis in axes:
        for apart in range(lax.axis_size(axis).bit_length() - 1):
            x = x + partner(x, axis, apart)
    return x


def bit_length(numbers, count):
    total = jnp.zeros_like(numbers)
    for place in range(count):
        total = total + (jnp.right_shift(numbers, place) > 0).astype(jnp.int32)
    return total


def level_table(level_weight, head_size):
    levels = jnp.arange(level_weight.shape[0], dtype=jnp.float32)
    factor = jnp.exp2(-0.5 * levels) / (8.0 * math.sqrt(head_size))
    return level_weight.astype(jnp.float32) * factor[:, None]


def lookup(level, table):
    onehot = (level[..., None] == jnp.arange(table.shape[0], dtype=jnp.int32)).astype(jnp.float32)
    flat = onehot.reshape(-1, table.shape[0])
    picked = jnp.dot(flat, table, precision=lax.Precision.HIGHEST)
    return picked.reshape(level.shape + (table.shape[1],))


def dot(a, b, da, db):
    return lax.dot_general(a, b, (((da,), (db,)), ((), ())), preferred_element_type=jnp.float32)


def tile_of(length):
    return min(256, length)


def diagonal(table_ref, h, tile, key_major):
    row = lax.broadcasted_iota(jnp.int32, (tile, tile), 0)
    col = lax.broadcasted_iota(jnp.int32, (tile, tile), 1)
    apart = jnp.bitwise_xor(row, col)
    weight = jnp.full((tile, tile), table_ref[0, h], jnp.float32)
    for level in range(1, tile.bit_length()):
        weight = jnp.where(apart >= 1 << (level - 1), table_ref[level, h], weight)
    causal = row <= col if key_major else col <= row
    return jnp.where(causal, weight, jnp.float32(0.0))


def weighted(table_ref, h, diag, scores, own, first):
    tile = scores.shape[0]
    base = tile.bit_length() - 1
    parts = []
    for place in range(scores.shape[1] // tile):
        other = first + place
        block = scores[:, place * tile : (place + 1) * tile]
        if other == own:
            factor = diag
        else:
            factor = table_ref[base + (own ^ other).bit_length(), h]
        parts.append((factor * block).astype(jnp.bfloat16))
    return parts[0] if len(parts) == 1 else jnp.concatenate(parts, axis=1)


def across_sum(weight_ref, h, gathered_ref):
    total = weight_ref[0, h] * gathered_ref[0, 0].astype(jnp.float32)
    for span in range(1, gathered_ref.shape[0]):
        total = total + weight_ref[span, h] * gathered_ref[span, 0].astype(jnp.float32)
    return total.astype(jnp.bfloat16)


def sums_kernel(q_ref, k_ref, v_ref, g_ref, grads_ref, states_ref):
    states_ref[0] = dot(k_ref[...], v_ref[...], 0, 0).astype(jnp.bfloat16)
    grads_ref[0] = dot(q_ref[...], g_ref[...], 0, 0).astype(jnp.bfloat16)


def value_part_kernel(table_ref, q_ref, k_ref, g_ref, part_ref):
    h = pl.program_id(0)
    tile = tile_of(q_ref.shape[0])
    diag = diagonal(table_ref, h, tile, True)
    for j in range(q_ref.shape[0] // tile):
        rows = slice(j * tile, (j + 1) * tile)
        later = slice(j * tile, q_ref.shape[0])
        scores = dot(k_ref[rows, :], q_ref[later, :], 1, 1)
        mixed = weighted(table_ref, h, diag, scores, j, j)
        part_ref[rows, :] = dot(mixed, g_ref[later, :], 1, 0)


def value_grad_kernel(returned_ref, k_ref, part_ref, grad_ref):
    grad_ref[...] = (part_ref[...] + dot(k_ref[...], returned_ref[0], 1, 0)).astype(jnp.bfloat16)


def query_key_kernel(
    table_ref, weight_ref, gathered_ref, returned_ref, q_ref, k_ref, v_ref, g_ref, dq_ref, dk_ref
):
    h = pl.program_id(0)
    length = q_ref.shape[0]
    tile = tile_of(length)
    carried = across_sum(weight_ref, h, gathered_ref)
    returned = returned_ref[0]
    by_key = diagonal(table_ref, h, tile, True)
    by_query = diagonal(table_ref, h, tile, False)
    for i in range(length // tile):
        rows = slice(i * tile, (i + 1) * tile)
        later = slice(i * tile, length)
        upto = slice(0, (i + 1) * tile)
        before = dot(v_ref[rows, :], g_ref[later, :], 1, 1)
        dmix = weighted(table_ref, h, by_key, before, i, i)
        key_grad = dot(dmix, q_ref[later, :], 1, 0) + dot(v_ref[rows, :], returned, 1, 1)
        dk_ref[rows, :] = key_grad.astype(jnp.bfloat16)
        before = dot(g_ref[rows, :], v_ref[upto, :], 1, 1)
        dmix = weighted(table_ref, h, by_query, before, i, 0)
        query_grad = dot(dmix, k_ref[upto, :], 1, 0) + dot(g_ref[rows, :], carried, 1, 1)
        dq_ref[rows, :] = query_grad.astype(jnp.bfloat16)


def proj_kernel(x_ref, grad_ref, out_ref):
    out_ref[...] = dot(x_ref[...], grad_ref[...], 0, 0).astype(jnp.bfloat16)


def cost(flops, nbytes):
    return pl.CostEstimate(flops=flops, bytes_accessed=nbytes, transcendentals=0)


def body(queries, keys, values, out_grad, inputs, momentum, level_weight):
    length, width = queries.shape
    per_dev = width // D_HEAD
    features = inputs.shape[1]
    table_all = level_table(level_weight, D_HEAD)
    table = lax.dynamic_slice_in_dim(table_all, lax.axis_index("head") * per_dev, per_dev, 1)
    rank = lax.axis_index("seq")
    spans = lax.axis_size("seq")
    base_level = length.bit_length() - 1
    sources = jnp.arange(spans, dtype=jnp.int32)
    level = bit_length(jnp.bitwise_xor(sources, rank), table.shape[0]) + base_level
    picked = lookup(level, table)
    state_weight = jnp.where((sources < rank)[:, None], picked, jnp.float32(0.0))

    smem = pl.BlockSpec(memory_space=pltpu.SMEM)
    rows = pl.BlockSpec((length, D_HEAD), lambda h: (0, h))
    matrix = pl.BlockSpec((1, D_HEAD, D_HEAD), lambda h: (h, 0, 0))
    everyone = pl.BlockSpec((spans, 1, D_HEAD, D_HEAD), lambda h: (0, h, 0, 0))
    matrices = jax.ShapeDtypeStruct((per_dev, D_HEAD, D_HEAD), jnp.bfloat16)
    narrow = jax.ShapeDtypeStruct((length, width), jnp.bfloat16)
    wide = jax.ShapeDtypeStruct((length, width), jnp.float32)
    once = 2 * length * width
    square = 2 * length * length * width

    grads, states = pl.pallas_call(
        sums_kernel,
        grid=(per_dev,),
        in_specs=[rows, rows, rows, rows],
        out_specs=(matrix, matrix),
        out_shape=(matrices, matrices),
        cost_estimate=cost(4 * length * width * D_HEAD, 4 * once),
    )(queries, keys, values, out_grad)
    all_states = lax.all_gather(states[None], "seq", axis=0, tiled=True)
    value_part = pl.pallas_call(
        value_part_kernel,
        grid=(per_dev,),
        in_specs=[smem, rows, rows, rows],
        out_specs=rows,
        out_shape=wide,
        cost_estimate=cost(4 * square, 5 * once),
    )(table, queries, keys, out_grad)
    block = grads.astype(jnp.float32)
    grad_sum = jnp.zeros(block.shape, jnp.float32)
    for bit in range(spans.bit_length() - 1):
        other = partner(block.astype(jnp.bfloat16), "seq", bit).astype(jnp.float32)
        weight = table[base_level + bit + 1][:, None, None]
        upper = jnp.bitwise_and(jnp.right_shift(rank, bit), 1) == 1
        grad_sum = grad_sum + jnp.where(upper, jnp.float32(0.0), weight * other)
        block = block + other
    returned = grad_sum.astype(jnp.bfloat16)
    value_grad = pl.pallas_call(
        value_grad_kernel,
        grid=(per_dev,),
        in_specs=[matrix, rows, rows],
        out_specs=rows,
        out_shape=narrow,
        cost_estimate=cost(2 * length * width * D_HEAD, 4 * once),
    )(returned, keys, value_part)
    step = min(256, features)
    partial = pl.pallas_call(
        proj_kernel,
        grid=(features // step,),
        in_specs=[
            pl.BlockSpec((length, step), lambda i: (0, i)),
            pl.BlockSpec((length, width), lambda i: (0, 0)),
        ],
        out_specs=pl.BlockSpec((step, width), lambda i: (i, 0)),
        out_shape=jax.ShapeDtypeStruct((features, width), jnp.bfloat16),
        cost_estimate=cost(2 * length * width * features, 2 * features * width + 2 * once),
    )(inputs, value_grad)
    partial, all_states = lax.optimization_barrier((partial, all_states))
    shard = lax.psum_scatter(partial, "seq", scatter_dimension=0, tiled=True).astype(jnp.float32)
    query_grad, key_grad = pl.pallas_call(
        query_key_kernel,
        grid=(per_dev,),
        in_specs=[smem, smem, everyone, matrix, rows, rows, rows, rows],
        out_specs=(rows, rows),
        out_shape=(narrow, narrow),
        cost_estimate=cost(8 * square, 10 * once),
    )(table, state_weight, all_states, returned, queries, keys, values, out_grad)
    total = sum_everywhere(jnp.sum(shard * shard), ("head", "seq"))
    factor = jnp.minimum(jnp.float32(1.0), clip_norm / jnp.sqrt(total + 1e-06))
    new_momentum = momentum_rate * momentum + factor * shard
    return (query_grad, key_grad, value_grad, new_momentum)


def solution(mesh):
    placed = (
        P("seq", "head"),
        P("seq", "head"),
        P("seq", "head"),
        P("seq", "head"),
        P("seq", None),
        P("seq", "head"),
        P(),
    )
    return jax.shard_map(
        body,
        mesh=mesh,
        in_specs=placed,
        out_specs=(P("seq", "head"), P("seq", "head"), P("seq", "head"), P("seq", "head")),
        check_vma=False,
    )
```
